32 devices in a mesh: wide: 8 (over y, x, core), narrow: 4 (over z).
Axes of the slice: x: 2, y: 2, z: 4, core: 2. Of those that a mesh axis runs over, the one named last changes fastest.
Arguments:
- hidden: bfloat16 [512, 4096], P('wide', 'narrow'), may hold values from -90 to 90
- head_weights: bfloat16 [4096, 303104], P(None, ('wide', 'narrow')), may hold values from -0.09375 to 0.09375
- token_ids: int32 [256], replicated, may hold values from 0 to 151551
- kl_weight: float32 [256], replicated, may hold values from 4 to 32
- advantage: float32 [256], replicated, may hold values from -12 to 12
Outputs:
- hidden_grad: float32 [4096, 512], P('narrow', 'wide')
- mixture_lse: float32 [256], replicated
- divergence: float32 [256], replicated
The draws below stay inside these ranges and needn't reach their ends.
All inputs are finite; a program needn't handle non-finite values.
Results may differ from the reference program's by a relative error of at most 0.012.
Values may be sent and summed in bfloat16 or wider, within the bound.
A program may use at most 192 MiB of HBM per device.

```python
import math
import jax
import jax.numpy as jnp
import numpy as np

D = 4096
VOCAB = 151552
TOKENS = 256


def draw_hidden(key, part):
    key_rows, key_cols = jax.random.split(jax.random.fold_in(key, 11))
    base = jnp.clip(jax.random.normal(key_cols, (2 * TOKENS, D), jnp.float32), -6.0, 6.0)
    scale = jnp.exp(jax.random.uniform(key_rows, (2 * TOKENS, 1), jnp.float32, 0.0, 2.4849066))
    return (base * scale).astype(jnp.bfloat16)


def touch_ends(drawn, key, least, high):
    shape = drawn.shape
    spot = [jax.random.randint(jax.random.fold_in(key, axis), (), 0, shape[axis]) for axis in range(len(shape))]
    drawn = drawn.at[tuple(spot)].set(least)
    longest = shape.index(max(shape))
    spot[longest] = (spot[longest] + 1) % shape[longest]
    return drawn.at[tuple(spot)].set(high)


def block_scale(own_key, dims, shards, least, top_value):
    gain, own = 1.0, jax.random.fold_in(own_key, 6)
    for dim, blocks in shards:
        heights = jnp.exp(jax.random.uniform(jax.random.fold_in(own, dim), (blocks,), jnp.float32, least / len(shards), top_value / len(shards)))
        gain = gain * jnp.repeat(heights, dims[dim] // blocks).reshape([-1 if axis == dim else 1 for axis in range(len(dims))])
    return gain


def wide_ids(rng, extent, number_of, slope):
    portions = [min(1 << octave, number_of + 1 - (1 << octave)) * (1 << 20) // math.isqrt((1 << octave) ** slope) + 1 for octave in range((number_of + 1).bit_length()) if 1 << octave <= number_of]
    scale = 1 + sum(portions) // (1 << 30)
    listing = np.cumsum(np.array([max(1, weight // scale) for weight in portions]))
    lot = jax.random.randint(jax.random.fold_in(rng, 1), extent, 0, int(listing[len(portions) - 1]))
    start = jnp.left_shift(1, jnp.searchsorted(jnp.asarray(listing, jnp.int32), lot, side="right").astype(jnp.int32))
    grade = start - 1 + jax.random.randint(jax.random.fold_in(rng, 4), extent, 0, 1 << 30) % jnp.minimum(start, number_of + 1 - start)
    return jax.random.permutation(jax.random.fold_in(rng, 2), number_of)[grade].astype(jnp.int32)


def gaussian(stream_key, extent, deviation, bound, pieces=(), kind=jnp.bfloat16):
    values = jax.random.normal(stream_key, extent, jnp.float32) * deviation
    if len(pieces) > 0:
        values = block_scale(stream_key, extent, pieces, -0.22, 0.18) * values
    return jnp.clip(values, min=-bound, max=bound).astype(kind)


def setup_inputs(seed: int = 0) -> dict:
    arg_keys = jax.random.split(jax.random.key(seed), 6)
    return {
        "hidden": draw_hidden(jax.random.fold_in(arg_keys[5], 71), 0),
        "head_weights": gaussian(arg_keys[1], (D, 2 * VOCAB), D ** -0.5, 0.09375, ((1, 32),)),
        "token_ids": touch_ends(wide_ids(arg_keys[2], (TOKENS,), VOCAB, 2), jax.random.fold_in(arg_keys[2], 3), 0, VOCAB - 1).astype(jnp.int32),
        "kl_weight": jnp.clip(jnp.exp(jax.random.uniform(arg_keys[3], (TOKENS,), jnp.float32, math.log(4.0), math.log(32.0))), 4.0, 32.0),
        "advantage": gaussian(arg_keys[4], (TOKENS,), 4.0, 12.0, (), jnp.float32),
    }


BETA = 0.2


def reference(hidden, head_weights, token_ids, kl_weight, advantage):
    policy_logits = jnp.dot(hidden[:TOKENS], head_weights[:, :VOCAB], preferred_element_type=jnp.float32)
    ref_logits = jnp.dot(hidden[TOKENS:], head_weights[:, VOCAB:], preferred_element_type=jnp.float32)
    mixed_logits = (1.0 - BETA) * policy_logits + BETA * ref_logits
    policy_lse = jax.nn.logsumexp(policy_logits, axis=1)
    mixture_lse = jax.nn.logsumexp(mixed_logits, axis=1)
    policy_prob = jnp.exp(policy_logits - policy_lse[:, None])
    mixture_prob = jnp.exp(mixed_logits - mixture_lse[:, None])
    log_gap = policy_logits - policy_lse[:, None] - mixed_logits + mixture_lse[:, None]
    divergence = jnp.sum(policy_prob * log_gap, axis=1)
    chosen = (token_ids[:, None] == jnp.arange(VOCAB, dtype=jnp.int32)[None, :]).astype(jnp.float32)
    prob_shift = mixture_prob - policy_prob
    policy_dlogits = (kl_weight[:, None] * (policy_prob * (log_gap - divergence[:, None]) + (1.0 - BETA) * prob_shift) - advantage[:, None] * (chosen - policy_prob)).astype(jnp.bfloat16)
    ref_dlogits = (BETA * kl_weight[:, None] * prob_shift).astype(jnp.bfloat16)
    grad_policy = jnp.dot(head_weights[:, :VOCAB], policy_dlogits.T, preferred_element_type=jnp.float32)
    grad_reference = jnp.dot(head_weights[:, VOCAB:], ref_dlogits.T, preferred_element_type=jnp.float32)
    hidden_grad = jnp.concatenate([grad_policy, grad_reference], axis=1)
    return hidden_grad, mixture_lse, divergence
```

```python
import functools

import jax
import jax.numpy as jnp
from jax import lax
from jax.experimental import pallas as pl
from jax.experimental.pallas import tpu as pltpu
from jax.sharding import PartitionSpec as P

BETA = 0.2
LANES = 128
CHUNKS = 4
WIDTH = 256
SLOTS = 6
AHEAD = 4
HIDDEN_MAX = 90.0
WEIGHT_MAX = 0.09375
MESH = pl.DeviceIdType.MESH
F32 = jnp.float32
BF16 = jnp.bfloat16


def partner(block, axis, bit):
    count = lax.axis_size(axis)
    route = []
    for low in range(count):
        high = low | 1 << bit
        if high != low and high < count:
            route += [(low, high), (high, low)]
    return lax.ppermute(block, axis, route)


def chunk_edges(width):
    blocks = -(-width // LANES)
    parts = min(CHUNKS, blocks)
    return [min(width, (blocks * i + parts - 1) // parts * LANES) for i in range(parts + 1)]


def body(hidden, head_weights, token_ids, kl_weight, advantage):
    wide_count = lax.axis_size("wide")
    narrow_count = lax.axis_size("narrow")
    half_count = wide_count // 2
    half_bits = half_count.bit_length() - 1
    wide_index = lax.axis_index("wide")
    narrow_index = lax.axis_index("narrow")
    is_reference = wide_index >= half_count
    block_width = head_weights.shape[1]
    col_start = (wide_index % half_count * narrow_count + narrow_index) * block_width
    edges = chunk_edges(block_width)
    spans = list(zip(edges[:-1], edges[1:]))

    gathered = lax.all_gather(hidden, "narrow", axis=1, tiled=True)
    for bit_number in reversed(range(half_bits)):
        partner_rows = partner(gathered, "wide", bit_number)
        upper_bit = wide_index // (1 << bit_number) % 2 == 1
        gathered = jnp.where(
            upper_bit,
            jnp.concatenate([partner_rows, gathered], 0),
            jnp.concatenate([gathered, partner_rows], 0),
        )
    row_total = gathered.shape[0]
    mid = row_total // 2

    def reverse_blocks(rows):
        split = rows.reshape((2,) * half_bits + (-1,))
        return split.transpose(tuple(reversed(range(half_bits))) + (half_bits,)).reshape(-1)

    def own_rows(rows):
        return jnp.where(is_reference, rows[mid:], rows[:mid])

    ids = own_rows(reverse_blocks(token_ids))[:, None]
    kl = own_rows(reverse_blocks(kl_weight))[:, None]
    adv = own_rows(reverse_blocks(advantage))[:, None]

    kept, received = [], []
    for low, high in spans:
        logits = jnp.dot(gathered, head_weights[:, low:high], preferred_element_type=jnp.float32)
        sent = jnp.where(is_reference, logits[:mid], logits[mid:])
        received.append(partner(sent, "wide", half_bits))
        kept.append(own_rows(logits))
    pairs, stats = [], []
    for own, other in zip(kept, received):
        policy = jnp.where(is_reference, other, own)
        ref = jnp.where(is_reference, own, other)
        mixed = (1.0 - BETA) * policy + BETA * ref
        p_top, m_top = jnp.max(policy, 1), jnp.max(mixed, 1)
        p_exp = jnp.exp(policy - p_top[:, None])
        m_exp = jnp.exp(mixed - m_top[:, None])
        stats.append(
            jnp.stack(
                [
                    p_top,
                    m_top,
                    jnp.sum(p_exp, 1),
                    jnp.sum(m_exp, 1),
                    jnp.sum(p_exp * (policy - mixed), 1),
                ]
            )
        )
        pairs.append((policy, mixed))

    def combine(parts):
        p_tops, m_tops, p_sums, m_sums, crosses = (parts[:, i] for i in range(5))
        p_top, m_top = jnp.max(p_tops, 0), jnp.max(m_tops, 0)
        p_scale, m_scale = jnp.exp(p_tops - p_top), jnp.exp(m_tops - m_top)
        return jnp.stack(
            [
                p_top,
                m_top,
                jnp.sum(p_sums * p_scale, 0),
                jnp.sum(m_sums * m_scale, 0),
                jnp.sum(crosses * p_scale, 0),
            ]
        )

    everyone = lax.all_gather(combine(jnp.stack(stats)), ("wide", "narrow"), axis=0, tiled=False)
    device_half = half_count * narrow_count
    total = jnp.concatenate(
        [combine(everyone[:device_half]), combine(everyone[device_half:])], 1
    )
    policy_lse_all = total[0] + jnp.log(total[2])
    mixture_lse_all = total[1] + jnp.log(total[3])
    divergence_all = total[4] / total[2] - policy_lse_all + mixture_lse_all
    policy_lse = own_rows(policy_lse_all)[:, None]
    mixture_lse = own_rows(mixture_lse_all)[:, None]
    divergence = own_rows(divergence_all)[:, None]

    own_grads, other_grads = [], []
    for (low, high), (policy, mixed) in zip(spans, pairs):
        policy_prob = jnp.exp(policy - policy_lse)
        mixture_prob = jnp.exp(mixed - mixture_lse)
        log_gap = policy - policy_lse - mixed + mixture_lse
        chosen = (
            ids == col_start + low + jnp.arange(high - low, dtype=jnp.int32)[None, :]
        ).astype(jnp.float32)
        prob_shift = mixture_prob - policy_prob
        policy_grad = (
            kl * (policy_prob * (log_gap - divergence) + (1.0 - BETA) * prob_shift)
            - adv * (chosen - policy_prob)
        ).astype(jnp.bfloat16)
        ref_grad = (BETA * kl * prob_shift).astype(jnp.bfloat16)
        own_grads.append(jnp.where(is_reference, ref_grad, policy_grad))
        other_grads.append(
            partner(jnp.where(is_reference, policy_grad, ref_grad), "wide", half_bits)
        )
    contract = (((1,), (1,)), ((), ()))
    summed = None
    for (low, high), own, other in zip(spans, own_grads, other_grads):
        grad = jnp.where(
            is_reference, jnp.concatenate([other, own], 0), jnp.concatenate([own, other], 0)
        )
        term = lax.dot_general(
            head_weights[:, low:high], grad, contract, preferred_element_type=jnp.float32
        )
        summed = term if summed is None else summed + term
    for bit_number in range(half_bits):
        half_size = summed.shape[1] // 2
        upper_bit = wide_index // (1 << bit_number) % 2 == 1
        kept_half = jnp.where(upper_bit, summed[:, half_size:], summed[:, :half_size])
        sent_half = jnp.where(upper_bit, summed[:, :half_size], summed[:, half_size:])
        summed = kept_half + partner(sent_half.astype(jnp.bfloat16), "wide", bit_number).astype(
            jnp.float32
        )
    summed = lax.psum_scatter(
        summed.astype(jnp.bfloat16), "narrow", scatter_dimension=0, tiled=True
    ).astype(jnp.float32)
    return (summed, reverse_blocks(mixture_lse_all), reverse_blocks(divergence_all))


def step_kernel(
    quarter, line, hid_ref, w_ref, ids_ref, kl_ref, adv_ref, grad_ref, row_ref,
    h_buf, w_buf, kept, send_q, recv_q, grads, send_d, top_buf, total,
    stat_send, stat_recv, fin_send, fin_recv,
    core_send, core_recv, x_send, x_recv, t_buf, up_send, up_recv, down_send, down_recv,
    w_sem, gz_up, gz_down, gz_recv, gx_send, gx_recv, gc_send, gc_recv,
    q_send_sem, q_recv_sem, d_send_sem, d_recv_sem, s_send_sem, s_recv_sem, f_sem,
    rc_send, rc_recv, rx_send, rx_recv, ru_send, ru_recv, rd_send, rd_recv,
):
    wide = lax.axis_index("wide")
    z = lax.axis_index("narrow")
    rows, feats = hid_ref.shape
    depth, width = w_ref.shape
    half = kept.shape[2]
    chunks = width // WIDTH
    sides = quarter // 2
    head = wide // quarter
    slot_q = wide % quarter
    x, core = slot_q // 2, slot_q % 2
    base = head * quarter
    is_ref = head == 1
    members = quarter * line
    me = slot_q * line + z

    def at(w, n):
        return {"wide": w, "narrow": n}

    across = at((wide + quarter) % (2 * quarter), z)
    x_side = at(base + (1 - x) * 2 + core, z)
    core_side = at(base + x * 2 + 1 - core, z)
    above, below = at(wide, z + 1), at(wide, z - 1)

    def peer(i):
        return at(base + i // line, i % line)

    def weights(t):
        col = pl.multiple_of(t % chunks * WIDTH, WIDTH)
        slot = t % SLOTS
        return pltpu.make_async_copy(w_ref.at[:, pl.ds(col, WIDTH)], w_buf.at[slot], w_sem.at[slot])

    for t in range(SLOTS - 1):
        weights(t).start()

    barrier = pltpu.get_barrier_semaphore()
    pl.semaphore_signal(barrier, inc=1, device_id=across, device_id_type=MESH)

    @pl.loop(1, members)
    def _(i):
        pl.semaphore_signal(
            barrier, inc=1, device_id=peer((me + i) % members), device_id_type=MESH
        )

    pl.semaphore_wait(barrier, members)

    def place(cx, cc, cz):
        pos = (cc + head - 2 * cc * head) * sides + cx
        return h_buf.at[
            pl.ds(pl.multiple_of(pos * rows, rows), rows),
            pl.ds(pl.multiple_of(cz * feats, feats), feats),
        ]

    def push(cx, cc, cz, own, send, recv, to):
        src = hid_ref if own else place(cx, cc, cz)
        return pltpu.make_async_remote_copy(
            src_ref=src, dst_ref=place(cx, cc, cz), send_sem=send, recv_sem=recv,
            device_id=to, device_id_type=MESH,
        )

    def g_up(cz, own=False):
        return push(x, core, cz, own, gz_up.at[cz], gz_recv.at[cz], above)

    def g_down(cz, own=False):
        return push(x, core, cz, own, gz_down.at[cz], gz_recv.at[cz], below)

    def g_x(cz, own=False):
        return push(x, core, cz, own, gx_send.at[cz], gx_recv.at[cz], x_side)

    def g_x_in(cz):
        return push(1 - x, core, cz, False, gx_send.at[cz], gx_recv.at[cz], x_side)

    def g_c(cx, cz, own=False):
        return push(cx, core, cz, own, gc_send.at[cx, cz], gc_recv.at[cx, cz], core_side)

    def g_c_in(cx, cz):
        return push(cx, 1 - core, cz, False, gc_send.at[cx, cz], gc_recv.at[cx, cz], core_side)

    @pl.when(z < line - 1)
    def _():
        g_up(z, True).start()

    @pl.when(z > 0)
    def _():
        g_down(z, True).start()

    g_x(z, True).start()
    g_c(x, z, True).start()
    place(x, core, z)[...] = hid_ref[...]

    def from_x(cz):
        g_x_in(cz).wait_recv()
        g_c(1 - x, cz).start()

    for s in range(1, line):
        @pl.when(z - s >= 0)
        def _():
            g_up(z - s).wait_recv()

            @pl.when(z < line - 1)
            def _():
                g_up(z - s).start()

            g_x(z - s).start()
            g_c(x, z - s).start()

        @pl.when(z + s < line)
        def _():
            g_down(z + s).wait_recv()

            @pl.when(z > 0)
            def _():
                g_down(z + s).start()

            g_x(z + s).start()
            g_c(x, z + s).start()

        if s == 1:
            from_x(z)
        else:
            @pl.when(z - s + 1 >= 0)
            def _():
                from_x(z - s + 1)

            @pl.when(z + s - 1 < line)
            def _():
                from_x(z + s - 1)

    last = line - 1

    if last > 0:
        @pl.when(z - last >= 0)
        def _():
            from_x(z - last)

        @pl.when(z + last < line)
        def _():
            from_x(z + last)
    else:
        from_x(z)

    total[...] = jnp.zeros_like(total)
    top_buf[...] = jnp.full_like(top_buf, -1e30)
    for cz in range(line):
        for cx in range(sides):
            g_c_in(cx, cz).wait_recv()

    reach = 2.0 * depth * HIDDEN_MAX * WEIGHT_MAX + 2.0
    code_scale = float(int(65500.0 / reach ** 0.25))

    def q_copy(j):
        return pltpu.make_async_remote_copy(
            src_ref=send_q.at[j], dst_ref=recv_q.at[j], send_sem=q_send_sem.at[j],
            recv_sem=q_recv_sem.at[j], device_id=across, device_id_type=MESH,
        )

    @pl.loop(0, chunks)
    def _(j):
        weights(j + SLOTS - 1).start()
        weights(j).wait()
        logits = jnp.dot(h_buf[...], w_buf[j % SLOTS], preferred_element_type=F32)
        kept[j] = logits[:half].T
        other = logits[half:].T
        top = jnp.maximum(top_buf[...], jnp.max(other, 0, keepdims=True))
        top_buf[...] = top
        top_code = jnp.floor(top * 0.5) + 1.0
        gap = jnp.sqrt(jnp.sqrt(jnp.maximum(2.0 * top_code[0:1] - other, 0.0)))
        code = (gap * code_scale + 0.5).astype(jnp.int32) - 32768
        send_q[j, 0:WIDTH] = code.astype(jnp.int16)
        send_q[j, WIDTH:] = jnp.broadcast_to(
            top_code[0:1].astype(jnp.int32), (16, half)
        ).astype(jnp.int16)

        @pl.when(j > 0)
        def _():
            q_copy(j - 1).start()

    q_copy(chunks - 1).start()

    def load_pair(j):
        own = kept[j]
        code = recv_q[j, 0:WIDTH].astype(jnp.int32).astype(F32) + 32768.0
        top = recv_q[j, WIDTH:].astype(jnp.int32).astype(F32)[0:1] * 2.0
        gap = code * (1.0 / code_scale)
        gap = gap * gap
        other = top - gap * gap
        policy = jnp.where(is_ref, other, own)
        ref = jnp.where(is_ref, own, other)
        return policy, (1.0 - BETA) * policy + BETA * ref

    def stat_step(j, carry):
        p_top, m_top, p_sum, m_sum, cross = carry
        q_copy(j).wait_recv()
        policy, mixed = load_pair(j)
        p_new = jnp.maximum(p_top, jnp.max(policy, 0, keepdims=True))
        m_new = jnp.maximum(m_top, jnp.max(mixed, 0, keepdims=True))
        p_exp, m_exp = jnp.exp(policy - p_new), jnp.exp(mixed - m_new)
        p_scale, m_scale = jnp.exp(p_top - p_new), jnp.exp(m_top - m_new)
        return (
            p_new,
            m_new,
            p_sum * p_scale + jnp.sum(p_exp, 0, keepdims=True),
            m_sum * m_scale + jnp.sum(m_exp, 0, keepdims=True),
            cross * p_scale + jnp.sum(p_exp * (policy - mixed), 0, keepdims=True),
        )

    low = jnp.full((1, half), -1e30, F32)
    zero = jnp.zeros((1, half), F32)
    stats = lax.fori_loop(0, chunks, stat_step, (low, low, zero, zero, zero))

    packed = jnp.concatenate(list(stats) + [zero, zero, zero], 0)
    stat_send[...] = packed
    stat_recv[me] = packed

    def s_copy(i):
        return pltpu.make_async_remote_copy(
            src_ref=stat_send, dst_ref=stat_recv.at[me], send_sem=s_send_sem.at[i],
            recv_sem=s_recv_sem.at[me], device_id=peer(i), device_id_type=MESH,
        )

    def s_copy_in(i):
        return pltpu.make_async_remote_copy(
            src_ref=stat_send, dst_ref=stat_recv.at[i], send_sem=s_send_sem.at[i],
            recv_sem=s_recv_sem.at[i], device_id=peer(i), device_id_type=MESH,
        )

    @pl.loop(1, members)
    def _(i):
        s_copy((me + i) % members).start()

    @pl.loop(1, members)
    def _(i):
        s_copy_in((me + i) % members).wait_recv()

    p_top, m_top = low, low
    for i in range(members):
        p_top = jnp.maximum(p_top, stat_recv[i, 0:1])
        m_top = jnp.maximum(m_top, stat_recv[i, 1:2])
    p_sum, m_sum, cross = zero, zero, zero
    for i in range(members):
        p_scale = jnp.exp(stat_recv[i, 0:1] - p_top)
        m_scale = jnp.exp(stat_recv[i, 1:2] - m_top)
        p_sum += stat_recv[i, 2:3] * p_scale
        m_sum += stat_recv[i, 3:4] * m_scale
        cross += stat_recv[i, 4:5] * p_scale
    policy_lse = p_top + jnp.log(p_sum)
    mixture_lse = m_top + jnp.log(m_sum)
    divergence = cross / p_sum - policy_lse + mixture_lse
    finals = jnp.concatenate([mixture_lse, divergence] + [zero] * 6, 0)
    fin_send[...] = finals

    kl = kl_ref[pl.ds(head, 1), :]
    adv = adv_ref[pl.ds(head, 1), :]
    ids = ids_ref[pl.ds(head, 1), :] - me * width
    col = lax.broadcasted_iota(jnp.int32, (WIDTH, half), 0)

    def d_copy(j):
        return pltpu.make_async_remote_copy(
            src_ref=send_d.at[j], dst_ref=grads.at[j, 1], send_sem=d_send_sem.at[j],
            recv_sem=d_recv_sem.at[j], device_id=across, device_id_type=MESH,
        )

    def grad_step(j):
        policy, mixed = load_pair(j)
        policy_prob = jnp.exp(policy - policy_lse)
        mixture_prob = jnp.exp(mixed - mixture_lse)
        log_gap = policy - policy_lse - mixed + mixture_lse
        chosen = jnp.where(col + j * WIDTH == ids, 1.0, 0.0)
        shift = mixture_prob - policy_prob
        policy_grad = kl * (
            policy_prob * (log_gap - divergence) + (1.0 - BETA) * shift
        ) - adv * (chosen - policy_prob)
        ref_grad = BETA * kl * shift
        grads[j, 0] = jnp.where(is_ref, ref_grad, policy_grad).astype(BF16)
        send_d[j] = jnp.where(is_ref, policy_grad, ref_grad).astype(BF16)

        @pl.when(j > 0)
        def _():
            d_copy(j - 1).start()

        @pl.when(j == chunks - 1)
        def _():
            d_copy(j).start()

    @pl.loop(0, min(AHEAD, chunks))
    def _(j):
        grad_step(j)

    f_copy = pltpu.make_async_remote_copy(
        src_ref=fin_send, dst_ref=fin_recv, send_sem=f_sem.at[0], recv_sem=f_sem.at[1],
        device_id=across, device_id_type=MESH,
    )
    f_copy.start()

    block = depth // 8

    @pl.loop(0, chunks)
    def _(j):
        @pl.when(j + AHEAD < chunks)
        def _():
            grad_step(j + AHEAD)

        @pl.when(j + SLOTS - 1 < chunks)
        def _():
            weights(chunks + j + SLOTS - 1).start()

        weights(chunks + j).wait()
        d_copy(j).wait_recv()
        rhs = jnp.concatenate([grads[j, 0], grads[j, 1]], 1)
        slot = (chunks + j) % SLOTS

        @pl.loop(0, 8)
        def _(b):
            span = pl.ds(pl.multiple_of(b * block, block), block)
            term = jnp.dot(w_buf[slot, span], rhs, preferred_element_type=F32)
            total[0, span] += term[:, :half]
            total[1, span] += term[:, half:]

    mine = core + head - 2 * core * head
    fold = feats // 2
    lane = lax.broadcasted_iota(jnp.int32, (fold, half), 1)

    def order(k):
        falling = line - 1 - k
        falling = falling - jnp.where(falling <= z, 1, 0)
        rising = k + jnp.where(k >= z, 1, 0)
        pick = jnp.where(z < line // 2, falling, rising)
        return jnp.where(k == line - 1, z, pick)

    def span_of(cz, part=None):
        if part is None:
            return pl.ds(pl.multiple_of(cz * feats, feats), feats)
        return pl.ds(pl.multiple_of(cz * feats + part * fold, fold), fold)

    def hand(src, dst, send, recv, to):
        return pltpu.make_async_remote_copy(
            src_ref=src, dst_ref=dst, send_sem=send, recv_sem=recv,
            device_id=to, device_id_type=MESH,
        )

    def r_core(cz):
        return hand(core_send.at[cz], core_recv.at[cz], rc_send.at[cz], rc_recv.at[cz], core_side)

    def r_x(cz):
        return hand(x_send.at[cz], x_recv.at[cz], rx_send.at[cz], rx_recv.at[cz], x_side)

    def r_up(cz):
        return hand(up_send.at[cz], up_recv.at[cz], ru_send.at[cz], ru_recv.at[cz], above)

    def r_down(cz):
        return hand(down_send.at[cz], down_recv.at[cz], rd_send.at[cz], rd_recv.at[cz], below)

    @pl.loop(0, line)
    def _(k):
        cz = order(k)
        core_send[cz] = total[1 - mine, span_of(cz)].astype(BF16)
        r_core(cz).start()

    @pl.loop(0, line)
    def _(k):
        cz = order(k)
        r_core(cz).wait_recv()
        upper = total[mine, span_of(cz, 0)] + core_recv[cz, 0:fold].astype(F32)
        lower = total[mine, span_of(cz, 1)] + core_recv[cz, fold:].astype(F32)
        left = jnp.where(lane < rows, upper, pltpu.roll(lower, rows, 1))
        right = jnp.where(lane < rows, pltpu.roll(upper, rows, 1), lower)
        t_buf[cz] = jnp.where(x == 0, left, right)
        x_send[cz] = jnp.where(x == 0, right, left).astype(BF16)
        r_x(cz).start()

    def settled(cz):
        r_x(cz).wait_recv()
        t_buf[cz] += x_recv[cz].astype(F32)

    def go_up(cz):
        settled(cz)

        @pl.when(z > 0)
        def _():
            r_up(cz).wait_recv()
            t_buf[cz] += up_recv[cz].astype(F32)

        up_send[cz] = t_buf[cz].astype(BF16)
        r_up(cz).start()

    def go_down(cz):
        settled(cz)

        @pl.when(z < line - 1)
        def _():
            r_down(cz).wait_recv()
            t_buf[cz] += down_recv[cz].astype(F32)

        down_send[cz] = t_buf[cz].astype(BF16)
        r_down(cz).start()

    @pl.loop(0, line - 1)
    def _(i):
        @pl.when(line - 1 - i > z)
        def _():
            go_up(line - 1 - i)

        @pl.when(i < z)
        def _():
            go_down(i)

    settled(z)

    @pl.when(z > 0)
    def _():
        r_up(z).wait_recv()
        t_buf[z] += up_recv[z].astype(F32)

    @pl.when(z < line - 1)
    def _():
        r_down(z).wait_recv()
        t_buf[z] += down_recv[z].astype(F32)

    done = t_buf[z]
    grad_ref[0:fold] = done[:, 0:rows]
    grad_ref[fold:] = pltpu.roll(done, rows, 1)[:, 0:rows]

    f_copy.wait_recv()
    theirs = fin_recv[...]
    row_ref[0] = jnp.where(is_ref, theirs, finals)
    row_ref[1] = jnp.where(is_ref, finals, theirs)

    f_copy.wait_send()

    @pl.loop(0, chunks)
    def _(j):
        q_copy(j).wait_send()
        d_copy(j).wait_send()

    @pl.loop(1, members)
    def _(i):
        s_copy((me + i) % members).wait_send()

    @pl.loop(0, line)
    def _(cz):
        r_core(cz).wait_send()
        r_x(cz).wait_send()
        g_x(cz).wait_send()
        for cx in range(sides):
            g_c(cx, cz).wait_send()

        @pl.when(cz > z)
        def _():
            r_up(cz).wait_send()

        @pl.when(cz < z)
        def _():
            r_down(cz).wait_send()

        @pl.when(jnp.logical_and(cz <= z, z < line - 1))
        def _():
            g_up(cz).wait_send()

        @pl.when(jnp.logical_and(cz >= z, z > 0))
        def _():
            g_down(cz).wait_send()


def fused(hidden, head_weights, token_ids, kl_weight, advantage):
    quarter, line = lax.axis_size("wide") // 2, lax.axis_size("narrow")
    rows, feats = hidden.shape
    depth, width = head_weights.shape
    tokens = rows * quarter
    half, sides = tokens // 2, quarter // 2
    chunks, members, fold = width // WIDTH, quarter * line, feats // 2

    def split(values):
        return values.reshape(sides, 2, rows).transpose(1, 0, 2).reshape(2, half)

    def join(values):
        return values.reshape(2, sides, rows).transpose(1, 0, 2).reshape(tokens)

    vmem = pl.BlockSpec(memory_space=pltpu.VMEM)
    dma, v = pltpu.SemaphoreType.DMA, pltpu.VMEM
    grad, per_row = pl.pallas_call(
        functools.partial(step_kernel, quarter, line),
        out_shape=(
            jax.ShapeDtypeStruct((feats, rows), F32),
            jax.ShapeDtypeStruct((2, 8, half), F32),
        ),
        in_specs=[vmem, pl.BlockSpec(memory_space=pl.ANY), vmem, vmem, vmem],
        out_specs=(vmem, vmem),
        scratch_shapes=[
            v((tokens, depth), BF16),
            v((SLOTS, depth, WIDTH), BF16),
            v((chunks, WIDTH, half), F32),
            v((chunks, WIDTH + 16, half), jnp.int16),
            v((chunks, WIDTH + 16, half), jnp.int16),
            v((chunks, 2, WIDTH, half), BF16),
            v((chunks, WIDTH, half), BF16),
            v((8, half), F32),
            v((2, depth, half), F32),
            v((8, half), F32),
            v((members, 8, half), F32),
            v((8, half), F32),
            v((8, half), F32),
            v((line, feats, half), BF16),
            v((line, feats, half), BF16),
            v((line, fold, half), BF16),
            v((line, fold, half), BF16),
            v((line, fold, half), F32),
            v((line, fold, half), BF16),
            v((line, fold, half), BF16),
            v((line, fold, half), BF16),
            v((line, fold, half), BF16),
            dma((SLOTS,)),
            dma((line,)), dma((line,)), dma((line,)), dma((line,)), dma((line,)),
            dma((sides, line)), dma((sides, line)),
            dma((chunks,)), dma((chunks,)), dma((chunks,)), dma((chunks,)),
            dma((members,)), dma((members,)), dma((2,)),
            dma((line,)), dma((line,)), dma((line,)), dma((line,)),
            dma((line,)), dma((line,)), dma((line,)), dma((line,)),
        ],
        compiler_params=pltpu.CompilerParams(
            collective_id=0, has_side_effects=True, vmem_limit_bytes=62 * 1024 * 1024
        ),
        name="step",
    )(hidden, head_weights, split(token_ids), split(kl_weight), split(advantage))
    return grad, join(per_row[:, 0]), join(per_row[:, 1])


def fits(quarter, line, hidden, head_weights):
    rows, feats = hidden.shape
    depth, width = head_weights.shape
    return (
        quarter == 4
        and line >= 2
        and rows * quarter == 2 * LANES
        and width % WIDTH == 0
        and width // WIDTH >= SLOTS
        and depth % (8 * LANES) == 0
        and feats % 32 == 0
        and feats * line == depth
    )


def device_step(hidden, head_weights, token_ids, kl_weight, advantage):
    quarter, line = lax.axis_size("wide") // 2, lax.axis_size("narrow")
    run = fused if fits(quarter, line, hidden, head_weights) else body
    return run(hidden, head_weights, token_ids, kl_weight, advantage)


def solution(mesh):
    return jax.shard_map(
        device_step,
        mesh=mesh,
        in_specs=(P("wide", "narrow"), P(None, ("wide", "narrow")), P(), P(), P()),
        out_specs=(P("narrow", "wide"), P(), P()),
        check_vma=False,
    )
```

```python
import functools

import jax
import jax.numpy as jnp
from jax import lax
from jax.experimental import pallas as pl
from jax.experimental.pallas import tpu as pltpu
from jax.sharding import PartitionSpec as P

BETA = 0.2
LANES = 128
CHUNKS = 4
WIDTH = 256
HELD = 8
RING = 4
BOTH = 6
PIECES = 2
AHEAD = 4
HIDDEN_MAX = 90.0
WEIGHT_MAX = 0.09375
MESH = pl.DeviceIdType.MESH
F32 = jnp.float32
BF16 = jnp.bfloat16


def partner(block, axis, bit):
    count = lax.axis_size(axis)
    route = []
    for low in range(count):
        high = low | 1 << bit
        if high != low and high < count:
            route += [(low, high), (high, low)]
    return lax.ppermute(block, axis, route)


def chunk_edges(width):
    blocks = -(-width // LANES)
    parts = min(CHUNKS, blocks)
    return [min(width, (blocks * i + parts - 1) // parts * LANES) for i in range(parts + 1)]


def body(hidden, head_weights, token_ids, kl_weight, advantage):
    wide_count = lax.axis_size("wide")
    narrow_count = lax.axis_size("narrow")
    half_count = wide_count // 2
    half_bits = half_count.bit_length() - 1
    wide_index = lax.axis_index("wide")
    narrow_index = lax.axis_index("narrow")
    is_reference = wide_index >= half_count
    block_width = head_weights.shape[1]
    col_start = (wide_index % half_count * narrow_count + narrow_index) * block_width
    edges = chunk_edges(block_width)
    spans = list(zip(edges[:-1], edges[1:]))

    gathered = lax.all_gather(hidden, "narrow", axis=1, tiled=True)
    for bit_number in reversed(range(half_bits)):
        partner_rows = partner(gathered, "wide", bit_number)
        upper_bit = wide_index // (1 << bit_number) % 2 == 1
        gathered = jnp.where(
            upper_bit,
            jnp.concatenate([partner_rows, gathered], 0),
            jnp.concatenate([gathered, partner_rows], 0),
        )
    row_total = gathered.shape[0]
    mid = row_total // 2

    def reverse_blocks(rows):
        split = rows.reshape((2,) * half_bits + (-1,))
        return split.transpose(tuple(reversed(range(half_bits))) + (half_bits,)).reshape(-1)

    def own_rows(rows):
        return jnp.where(is_reference, rows[mid:], rows[:mid])

    ids = own_rows(reverse_blocks(token_ids))[:, None]
    kl = own_rows(reverse_blocks(kl_weight))[:, None]
    adv = own_rows(reverse_blocks(advantage))[:, None]

    kept, received = [], []
    for low, high in spans:
        logits = jnp.dot(gathered, head_weights[:, low:high], preferred_element_type=jnp.float32)
        sent = jnp.where(is_reference, logits[:mid], logits[mid:])
        received.append(partner(sent, "wide", half_bits))
        kept.append(own_rows(logits))
    pairs, stats = [], []
    for own, other in zip(kept, received):
        policy = jnp.where(is_reference, other, own)
        ref = jnp.where(is_reference, own, other)
        mixed = (1.0 - BETA) * policy + BETA * ref
        p_top, m_top = jnp.max(policy, 1), jnp.max(mixed, 1)
        p_exp = jnp.exp(policy - p_top[:, None])
        m_exp = jnp.exp(mixed - m_top[:, None])
        stats.append(
            jnp.stack(
                [
                    p_top,
                    m_top,
                    jnp.sum(p_exp, 1),
                    jnp.sum(m_exp, 1),
                    jnp.sum(p_exp * (policy - mixed), 1),
                ]
            )
        )
        pairs.append((policy, mixed))

    def combine(parts):
        p_tops, m_tops, p_sums, m_sums, crosses = (parts[:, i] for i in range(5))
        p_top, m_top = jnp.max(p_tops, 0), jnp.max(m_tops, 0)
        p_scale, m_scale = jnp.exp(p_tops - p_top), jnp.exp(m_tops - m_top)
        return jnp.stack(
            [
                p_top,
                m_top,
                jnp.sum(p_sums * p_scale, 0),
                jnp.sum(m_sums * m_scale, 0),
                jnp.sum(crosses * p_scale, 0),
            ]
        )

    everyone = lax.all_gather(combine(jnp.stack(stats)), ("wide", "narrow"), axis=0, tiled=False)
    device_half = half_count * narrow_count
    total = jnp.concatenate(
        [combine(everyone[:device_half]), combine(everyone[device_half:])], 1
    )
    policy_lse_all = total[0] + jnp.log(total[2])
    mixture_lse_all = total[1] + jnp.log(total[3])
    divergence_all = total[4] / total[2] - policy_lse_all + mixture_lse_all
    policy_lse = own_rows(policy_lse_all)[:, None]
    mixture_lse = own_rows(mixture_lse_all)[:, None]
    divergence = own_rows(divergence_all)[:, None]

    own_grads, other_grads = [], []
    for (low, high), (policy, mixed) in zip(spans, pairs):
        policy_prob = jnp.exp(policy - policy_lse)
        mixture_prob = jnp.exp(mixed - mixture_lse)
        log_gap = policy - policy_lse - mixed + mixture_lse
        chosen = (
            ids == col_start + low + jnp.arange(high - low, dtype=jnp.int32)[None, :]
        ).astype(jnp.float32)
        prob_shift = mixture_prob - policy_prob
        policy_grad = (
            kl * (policy_prob * (log_gap - divergence) + (1.0 - BETA) * prob_shift)
            - adv * (chosen - policy_prob)
        ).astype(jnp.bfloat16)
        ref_grad = (BETA * kl * prob_shift).astype(jnp.bfloat16)
        own_grads.append(jnp.where(is_reference, ref_grad, policy_grad))
        other_grads.append(
            partner(jnp.where(is_reference, policy_grad, ref_grad), "wide", half_bits)
        )
    contract = (((1,), (1,)), ((), ()))
    summed = None
    for (low, high), own, other in zip(spans, own_grads, other_grads):
        grad = jnp.where(
            is_reference, jnp.concatenate([other, own], 0), jnp.concatenate([own, other], 0)
        )
        term = lax.dot_general(
            head_weights[:, low:high], grad, contract, preferred_element_type=jnp.float32
        )
        summed = term if summed is None else summed + term
    for bit_number in range(half_bits):
        half_size = summed.shape[1] // 2
        upper_bit = wide_index // (1 << bit_number) % 2 == 1
        kept_half = jnp.where(upper_bit, summed[:, half_size:], summed[:, :half_size])
        sent_half = jnp.where(upper_bit, summed[:, :half_size], summed[:, half_size:])
        summed = kept_half + partner(sent_half.astype(jnp.bfloat16), "wide", bit_number).astype(
            jnp.float32
        )
    summed = lax.psum_scatter(
        summed.astype(jnp.bfloat16), "narrow", scatter_dimension=0, tiled=True
    ).astype(jnp.float32)
    return (summed, reverse_blocks(mixture_lse_all), reverse_blocks(divergence_all))


def step_kernel(
    quarter, line, hid_ref, w_ref, ids_ref, kl_ref, adv_ref, grad_ref, lse_ref, div_ref,
    h_buf, w_buf, kept, kept_x, send_q, recv_q, send_x, recv_x, grads, send_d, top_buf, total,
    stat_send, stat_recv, fin_send, fin_recv,
    core_send, core_recv, x_send, x_recv, t_buf, z_send, z_recv,
    w_sem, gz_up, gz_down, gz_recv, gx_send, gx_recv, gc_send, gc_recv,
    q_send_sem, q_recv_sem, e_send_sem, e_recv_sem, d_send_sem, d_recv_sem, s_send_sem, s_recv_sem, f_sem,
    rc_send, rc_recv, rx_send, rx_recv, rz_send, rz_recv,
):
    wide = lax.axis_index("wide")
    z = lax.axis_index("narrow")
    rows, feats = hid_ref.shape
    depth, width = w_ref.shape
    half = kept.shape[2]
    chunks = width // WIDTH
    sides = quarter // 2
    head = wide // quarter
    slot_q = wide % quarter
    x, core = slot_q // 2, slot_q % 2
    base = head * quarter
    is_ref = head == 1
    members = quarter * line
    me = slot_q * line + z

    def at(w, n):
        return {"wide": w, "narrow": n}

    across = at((wide + quarter) % (2 * quarter), z)
    x_side = at(base + (1 - x) * 2 + core, z)
    core_side = at(base + x * 2 + 1 - core, z)
    above, below = at(wide, z + 1), at(wide, z - 1)

    def peer(i):
        return at(base + i // line, i % line)

    passing = chunks - HELD

    def fetch(chunk, slot):
        col = pl.multiple_of(chunk * WIDTH, WIDTH)
        return pltpu.make_async_copy(w_ref.at[:, pl.ds(col, WIDTH)], w_buf.at[slot], w_sem.at[slot])

    def held(chunk):
        return fetch(chunk, RING + chunk)

    def weights(t):
        return fetch(HELD + t % passing, t % RING)

    @pl.loop(0, HELD)
    def _(c):
        held(c).start()

    for t in range(RING - 1):
        weights(t).start()

    barrier = pltpu.get_barrier_semaphore()
    for to in (core_side, x_side, across):
        pl.semaphore_signal(barrier, inc=1, device_id=to, device_id_type=MESH)

    @pl.when(z > 0)
    def _():
        pl.semaphore_signal(barrier, inc=1, device_id=below, device_id_type=MESH)

    @pl.when(z < line - 1)
    def _():
        pl.semaphore_signal(barrier, inc=1, device_id=above, device_id_type=MESH)

    at_end = jnp.logical_or(z == 0, z == line - 1)

    @pl.when(at_end)
    def _():
        pl.semaphore_wait(barrier, 4)

    @pl.when(jnp.logical_not(at_end))
    def _():
        pl.semaphore_wait(barrier, 5)

    piece = rows // PIECES

    def place(cx, cc, cz, p):
        pos = (cc + head - 2 * cc * head) * sides + cx
        return h_buf.at[
            pl.ds(pl.multiple_of(pos * rows + p * piece, piece), piece),
            pl.ds(pl.multiple_of(cz * feats, feats), feats),
        ]

    def push(cx, cc, cz, p, own, send, recv, to):
        src = hid_ref.at[pl.ds(p * piece, piece)] if own else place(cx, cc, cz, p)
        return pltpu.make_async_remote_copy(
            src_ref=src, dst_ref=place(cx, cc, cz, p), send_sem=send, recv_sem=recv,
            device_id=to, device_id_type=MESH,
        )

    def g_up(cz, p, own=False):
        return push(x, core, cz, p, own, gz_up.at[cz, p], gz_recv.at[cz, p], above)

    def g_down(cz, p, own=False):
        return push(x, core, cz, p, own, gz_down.at[cz, p], gz_recv.at[cz, p], below)

    def g_x(cz, p, own=False):
        return push(x, core, cz, p, own, gx_send.at[cz, p], gx_recv.at[cz, p], x_side)

    def g_x_in(cz, p):
        return push(1 - x, core, cz, p, False, gx_send.at[cz, p], gx_recv.at[cz, p], x_side)

    def g_c(cx, cz, p, own=False):
        return push(cx, core, cz, p, own, gc_send.at[cx, cz, p], gc_recv.at[cx, cz, p], core_side)

    def g_c_in(cx, cz, p):
        return push(
            cx, 1 - core, cz, p, False, gc_send.at[cx, cz, p], gc_recv.at[cx, cz, p], core_side
        )

    mine = core + head - 2 * core * head

    for p in range(PIECES):
        @pl.when(z < line - 1)
        def _():
            g_up(z, p, True).start()

        @pl.when(z > 0)
        def _():
            g_down(z, p, True).start()

        g_x(z, p, True).start()
        g_c(x, z, p, True).start()
        place(x, core, z, p)[...] = hid_ref[p * piece : (p + 1) * piece]

    total[...] = jnp.zeros_like(total)
    top_buf[...] = jnp.full_like(top_buf, -1e30)

    def from_x(cz, p):
        g_x_in(cz, p).wait_recv()
        g_c(1 - x, cz, p).start()

    for s in range(1, line + 1):
        for p in range(PIECES):
            if s < line:
                @pl.when(z - s >= 0)
                def _():
                    g_up(z - s, p).wait_recv()

                    @pl.when(z < line - 1)
                    def _():
                        g_up(z - s, p).start()

                    g_x(z - s, p).start()
                    g_c(x, z - s, p).start()

                @pl.when(z + s < line)
                def _():
                    g_down(z + s, p).wait_recv()

                    @pl.when(z > 0)
                    def _():
                        g_down(z + s, p).start()

                    g_x(z + s, p).start()
                    g_c(x, z + s, p).start()

            if s == 1:
                from_x(z, p)
            else:
                @pl.when(z - s + 1 >= 0)
                def _():
                    from_x(z - s + 1, p)

                @pl.when(z + s - 1 < line)
                def _():
                    from_x(z + s - 1, p)

    for cz in range(line):
        for cx in range(sides):
            for p in range(PIECES):
                g_c_in(cx, cz, p).wait_recv()

    reach = 2.0 * depth * HIDDEN_MAX * WEIGHT_MAX + 2.0
    code_scale = float(int(65500.0 / reach ** 0.25))

    def q_copy(j):
        return pltpu.make_async_remote_copy(
            src_ref=send_q.at[j], dst_ref=recv_q.at[j], send_sem=q_send_sem.at[j],
            recv_sem=q_recv_sem.at[j], device_id=across, device_id_type=MESH,
        )

    def extra_copy(i):
        return pltpu.make_async_remote_copy(
            src_ref=send_x.at[i], dst_ref=recv_x.at[i], send_sem=e_send_sem.at[i],
            recv_sem=e_recv_sem.at[i], device_id=across, device_id_type=MESH,
        )

    def encode(ref, j, values, top):
        top_code = jnp.floor(top * 0.5) + 1.0
        gap = jnp.sqrt(jnp.sqrt(jnp.maximum(2.0 * top_code - values, 0.0)))
        code = (gap * code_scale + 0.5).astype(jnp.int32) - 32768
        ref[j, 0:WIDTH] = code.astype(jnp.int16)
        ref[j, WIDTH:] = jnp.broadcast_to(top_code.astype(jnp.int32), (16, half)).astype(jnp.int16)

    def slot_of(j):
        return jnp.where(j < HELD, RING + j, (j - HELD) % RING)

    @pl.loop(0, chunks)
    def _(j):
        @pl.when(j < HELD)
        def _():
            held(j).wait()

        @pl.when(j >= HELD)
        def _():
            weights(j - HELD + RING - 1).start()
            weights(j - HELD).wait()

        logits = jnp.dot(h_buf[...], w_buf[slot_of(j)], preferred_element_type=F32)
        own, other = logits[:half].T, logits[half:].T
        kept[j] = own
        top = jnp.maximum(top_buf[...], jnp.max(other, 0, keepdims=True))
        top_buf[...] = top
        encode(send_q, j, other, top[0:1])

        @pl.when(jnp.logical_and(j >= HELD, j < HELD + BOTH))
        def _():
            kept_x[j - HELD] = other
            encode(send_x, j - HELD, own, jnp.max(own, 0, keepdims=True))

        @pl.when(j > 0)
        def _():
            q_copy(j - 1).start()

    q_copy(chunks - 1).start()

    @pl.loop(0, BOTH)
    def _(i):
        extra_copy(i).start()

    def pair(ours, ref, j):
        code = ref[j, 0:WIDTH].astype(jnp.int32).astype(F32) + 32768.0
        top = ref[j, WIDTH:].astype(jnp.int32).astype(F32)[0:1] * 2.0
        gap = code * (1.0 / code_scale)
        gap = gap * gap
        theirs = top - gap * gap
        policy = jnp.where(is_ref, theirs, ours)
        ref = jnp.where(is_ref, ours, theirs)
        return policy, (1.0 - BETA) * policy + BETA * ref

    def load_pair(j):
        return pair(kept[j], recv_q, j)

    def stat_step(j, carry):
        p_top, m_top, p_sum, m_sum, cross = carry
        q_copy(j).wait_recv()
        policy, mixed = load_pair(j)
        p_new = jnp.maximum(p_top, jnp.max(policy, 0, keepdims=True))
        m_new = jnp.maximum(m_top, jnp.max(mixed, 0, keepdims=True))
        p_exp, m_exp = jnp.exp(policy - p_new), jnp.exp(mixed - m_new)
        p_scale, m_scale = jnp.exp(p_top - p_new), jnp.exp(m_top - m_new)
        return (
            p_new,
            m_new,
            p_sum * p_scale + jnp.sum(p_exp, 0, keepdims=True),
            m_sum * m_scale + jnp.sum(m_exp, 0, keepdims=True),
            cross * p_scale + jnp.sum(p_exp * (policy - mixed), 0, keepdims=True),
        )

    low = jnp.full((1, half), -1e30, F32)
    zero = jnp.zeros((1, half), F32)
    stats = lax.fori_loop(0, chunks, stat_step, (low, low, zero, zero, zero))

    packed = jnp.concatenate(list(stats) + [zero, zero, zero], 0)
    stat_send[...] = packed
    stat_recv[me] = packed

    def s_copy(i):
        return pltpu.make_async_remote_copy(
            src_ref=stat_send, dst_ref=stat_recv.at[me], send_sem=s_send_sem.at[i],
            recv_sem=s_recv_sem.at[me], device_id=peer(i), device_id_type=MESH,
        )

    def s_copy_in(i):
        return pltpu.make_async_remote_copy(
            src_ref=stat_send, dst_ref=stat_recv.at[i], send_sem=s_send_sem.at[i],
            recv_sem=s_recv_sem.at[i], device_id=peer(i), device_id_type=MESH,
        )

    @pl.loop(1, members)
    def _(i):
        s_copy((me + i) % members).start()

    @pl.loop(1, members)
    def _(i):
        s_copy_in((me + i) % members).wait_recv()

    p_top, m_top = low, low
    for i in range(members):
        p_top = jnp.maximum(p_top, stat_recv[i, 0:1])
        m_top = jnp.maximum(m_top, stat_recv[i, 1:2])
    p_sum, m_sum, cross = zero, zero, zero
    for i in range(members):
        p_scale = jnp.exp(stat_recv[i, 0:1] - p_top)
        m_scale = jnp.exp(stat_recv[i, 1:2] - m_top)
        p_sum += stat_recv[i, 2:3] * p_scale
        m_sum += stat_recv[i, 3:4] * m_scale
        cross += stat_recv[i, 4:5] * p_scale
    policy_lse = p_top + jnp.log(p_sum)
    mixture_lse = m_top + jnp.log(m_sum)
    divergence = cross / p_sum - policy_lse + mixture_lse
    finals = jnp.concatenate([mixture_lse, divergence, policy_lse] + [zero] * 5, 0)
    fin_send[...] = finals

    place_lane = lax.broadcasted_iota(jnp.int32, (1, half), 1)

    def own_row(ref, second_half):
        first, second = ref[0:half].reshape(1, half), ref[half:].reshape(1, half)
        low_part = jnp.where(place_lane < rows, first, pltpu.roll(second, rows, 1))
        high_part = jnp.where(place_lane < rows, pltpu.roll(first, rows, 1), second)
        return jnp.where(second_half, high_part, low_part)

    base_col = me * width

    def row_values(second_half):
        return (
            own_row(kl_ref, second_half),
            own_row(adv_ref, second_half),
            own_row(ids_ref, second_half) - base_col,
        )

    ours = row_values(is_ref) + (policy_lse, mixture_lse, divergence)
    col = lax.broadcasted_iota(jnp.int32, (WIDTH, half), 0)

    def d_copy(j):
        return pltpu.make_async_remote_copy(
            src_ref=send_d.at[j], dst_ref=grads.at[j, 1], send_sem=d_send_sem.at[j],
            recv_sem=d_recv_sem.at[j], device_id=across, device_id_type=MESH,
        )

    def grads_of(j, policy, mixed, values):
        kl, adv, ids, p_lse, m_lse, div = values
        policy_prob = jnp.exp(policy - p_lse)
        mixture_prob = jnp.exp(mixed - m_lse)
        log_gap = policy - p_lse - mixed + m_lse
        chosen = jnp.where(col + j * WIDTH == ids, 1.0, 0.0)
        shift = mixture_prob - policy_prob
        policy_grad = kl * (
            policy_prob * (log_gap - div) + (1.0 - BETA) * shift
        ) - adv * (chosen - policy_prob)
        return policy_grad, BETA * kl * shift

    def grad_step(j):
        policy, mixed = load_pair(j)
        policy_grad, ref_grad = grads_of(j, policy, mixed, ours)
        grads[j, 0] = jnp.where(is_ref, ref_grad, policy_grad).astype(BF16)
        send_d[j] = jnp.where(is_ref, policy_grad, ref_grad).astype(BF16)

    first_sent = HELD + BOTH
    sent = passing - BOTH

    def send_grad(k):
        @pl.when(k < sent)
        def _():
            d_copy(first_sent + k).start()

        @pl.when(jnp.logical_and(k >= sent, k < sent + HELD))
        def _():
            d_copy(k - sent).start()

    f_copy = pltpu.make_async_remote_copy(
        src_ref=fin_send, dst_ref=fin_recv, send_sem=f_sem.at[0], recv_sem=f_sem.at[1],
        device_id=across, device_id_type=MESH,
    )

    @pl.loop(0, AHEAD)
    def _(k):
        grad_step(first_sent + k)

        @pl.when(k > 0)
        def _():
            d_copy(first_sent + k - 1).start()

        @pl.when(k == 0)
        def _():
            f_copy.start()

    def add(part, slot, rhs):
        total[part] += jnp.dot(w_buf[slot], rhs, preferred_element_type=F32)

    f_copy.wait_recv()
    row_stats = fin_recv[...]
    theirs = row_values(jnp.logical_not(is_ref)) + (
        row_stats[2:3], row_stats[0:1], row_stats[1:2]
    )

    @pl.loop(0, passing)
    def _(t):
        j = HELD + t
        k = t + AHEAD

        @pl.when(k < sent)
        def _():
            grad_step(first_sent + k)

        send_grad(k - 1)

        @pl.when(t + RING - 1 < passing)
        def _():
            weights(passing + t + RING - 1).start()

        weights(passing + t).wait()

        @pl.when(t < BOTH)
        def _():
            grad_step(j)
            extra_copy(t).wait_recv()
            policy, mixed = pair(kept_x[t], recv_x, t)
            policy_grad, ref_grad = grads_of(j, policy, mixed, theirs)
            grads[j, 1] = jnp.where(is_ref, ref_grad, policy_grad).astype(BF16)

        @pl.when(jnp.logical_and(t >= BOTH, t < BOTH + HELD))
        def _():
            grad_step(t - BOTH)
            add(0, RING + t - BOTH, grads[t - BOTH, 0])

        @pl.when(t >= BOTH)
        def _():
            d_copy(j).wait_recv()

        rhs = jnp.concatenate([grads[j, 0], grads[j, 1]], 1)
        term = jnp.dot(w_buf[(passing + t) % RING], rhs, preferred_element_type=F32)
        total[0] += term[:, :half]
        total[1] += term[:, half:]

    fold = feats // 2
    lane = lax.broadcasted_iota(jnp.int32, (fold, half), 1)

    def order(k):
        falling = line - 1 - k
        falling = falling - jnp.where(falling <= z, 1, 0)
        rising = k + jnp.where(k >= z, 1, 0)
        pick = jnp.where(z < line // 2, falling, rising)
        return jnp.where(k == line - 1, z, pick)

    def span_of(cz, part=None):
        if part is None:
            return pl.ds(pl.multiple_of(cz * feats, feats), feats)
        return pl.ds(pl.multiple_of(cz * feats + part * fold, fold), fold)

    def hand(src, dst, send, recv, to):
        return pltpu.make_async_remote_copy(
            src_ref=src, dst_ref=dst, send_sem=send, recv_sem=recv,
            device_id=to, device_id_type=MESH,
        )

    def r_core(cz):
        return hand(core_send.at[cz], core_recv.at[cz], rc_send.at[cz], rc_recv.at[cz], core_side)

    def r_x(cz):
        return hand(x_send.at[cz], x_recv.at[cz], rx_send.at[cz], rx_recv.at[cz], x_side)

    def r_z(cz):
        return hand(z_send.at[cz], z_recv.at[z], rz_send.at[cz], rz_recv.at[z], at(wide, cz))

    def r_z_in(cz):
        return hand(z_send.at[cz], z_recv.at[cz], rz_send.at[cz], rz_recv.at[cz], at(wide, cz))

    def to_core(k):
        cz = order(k)
        core_send[cz] = total[1 - mine, span_of(cz)].astype(BF16)
        r_core(cz).start()

    def to_x(k):
        cz = order(k)
        r_core(cz).wait_recv()
        upper = total[mine, span_of(cz, 0)] + core_recv[cz, 0:fold].astype(F32)
        lower = total[mine, span_of(cz, 1)] + core_recv[cz, fold:].astype(F32)
        left = jnp.where(lane < rows, upper, pltpu.roll(lower, rows, 1))
        right = jnp.where(lane < rows, pltpu.roll(upper, rows, 1), lower)
        t_buf[cz] = jnp.where(x == 0, left, right)
        x_send[cz] = jnp.where(x == 0, right, left).astype(BF16)
        r_x(cz).start()

    def to_z(k):
        cz = order(k)
        r_x(cz).wait_recv()
        z_send[cz] = (t_buf[cz] + x_recv[cz].astype(F32)).astype(BF16)
        r_z(cz).start()

    @pl.loop(0, HELD)
    def _(j):
        send_grad(passing + j + AHEAD - 1)

        @pl.when(jnp.logical_and(mine == 1, j == 0))
        def _():
            @pl.loop(0, line)
            def _(k):
                to_core(k)

        @pl.when(jnp.logical_and(mine == 0, jnp.logical_and(j >= 2, j < 2 + line)))
        def _():
            to_x(j - 2)

        @pl.when(jnp.logical_and(mine == 0, jnp.logical_and(j >= 5, j < 4 + line)))
        def _():
            to_z(j - 5)

        d_copy(j).wait_recv()
        add(1, RING + j, grads[j, 1])

    @pl.when(mine == 0)
    def _():
        @pl.loop(0, line)
        def _(k):
            to_core(k)

    @pl.when(mine == 1)
    def _():
        @pl.loop(0, line)
        def _(k):
            to_x(k)

        @pl.loop(0, line - 1)
        def _(k):
            to_z(k)

    r_x(z).wait_recv()
    t_buf[z] += x_recv[z].astype(F32)

    @pl.loop(1, line)
    def _(i):
        cz = (z + i) % line
        r_z_in(cz).wait_recv()
        t_buf[z] += z_recv[cz].astype(F32)

    done = t_buf[z]
    grad_ref[0:fold] = done[:, 0:rows]
    grad_ref[fold:] = pltpu.roll(done, rows, 1)[:, 0:rows]

    even, odd = jnp.where(is_ref, row_stats, finals), jnp.where(is_ref, finals, row_stats)
    wide_lane = lax.broadcasted_iota(jnp.int32, (8, half), 1)
    first = jnp.where(wide_lane < rows, even, pltpu.roll(odd, rows, 1))
    second = jnp.where(wide_lane < rows, pltpu.roll(even, rows, 1), odd)
    lse_ref[0:half] = first[0]
    lse_ref[half:] = second[0]
    div_ref[0:half] = first[1]
    div_ref[half:] = second[1]

    f_copy.wait_send()

    @pl.loop(0, chunks)
    def _(j):
        q_copy(j).wait_send()

        @pl.when(jnp.logical_or(j < HELD, j >= first_sent))
        def _():
            d_copy(j).wait_send()

    @pl.loop(0, BOTH)
    def _(i):
        extra_copy(i).wait_send()

    @pl.loop(1, members)
    def _(i):
        s_copy((me + i) % members).wait_send()

    @pl.loop(1, line)
    def _(i):
        r_z((z + i) % line).wait_send()

    @pl.loop(0, line)
    def _(cz):
        r_core(cz).wait_send()
        r_x(cz).wait_send()
        for p in range(PIECES):
            g_x(cz, p).wait_send()
            for cx in range(sides):
                g_c(cx, cz, p).wait_send()

            @pl.when(jnp.logical_and(cz <= z, z < line - 1))
            def _():
                g_up(cz, p).wait_send()

            @pl.when(jnp.logical_and(cz >= z, z > 0))
            def _():
                g_down(cz, p).wait_send()


def fused(hidden, head_weights, token_ids, kl_weight, advantage):
    quarter, line = lax.axis_size("wide") // 2, lax.axis_size("narrow")
    rows, feats = hidden.shape
    depth, width = head_weights.shape
    tokens = rows * quarter
    half, sides = tokens // 2, quarter // 2
    chunks, members, fold = width // WIDTH, quarter * line, feats // 2
    vmem = pl.BlockSpec(memory_space=pltpu.VMEM)
    dma, v = pltpu.SemaphoreType.DMA, pltpu.VMEM
    along = dma((line, PIECES))
    return pl.pallas_call(
        functools.partial(step_kernel, quarter, line),
        out_shape=(
            jax.ShapeDtypeStruct((feats, rows), F32),
            jax.ShapeDtypeStruct((tokens,), F32),
            jax.ShapeDtypeStruct((tokens,), F32),
        ),
        in_specs=[vmem, pl.BlockSpec(memory_space=pl.ANY), vmem, vmem, vmem],
        out_specs=(vmem, vmem, vmem),
        scratch_shapes=[
            v((tokens, depth), BF16),
            v((RING + HELD, depth, WIDTH), BF16),
            v((chunks, WIDTH, half), F32),
            v((BOTH, WIDTH, half), F32),
            v((chunks, WIDTH + 16, half), jnp.int16),
            v((chunks, WIDTH + 16, half), jnp.int16),
            v((BOTH, WIDTH + 16, half), jnp.int16),
            v((BOTH, WIDTH + 16, half), jnp.int16),
            v((chunks, 2, WIDTH, half), BF16),
            v((chunks, WIDTH, half), BF16),
            v((8, half), F32),
            v((2, depth, half), F32),
            v((8, half), F32),
            v((members, 8, half), F32),
            v((8, half), F32),
            v((8, half), F32),
            v((line, feats, half), BF16),
            v((line, feats, half), BF16),
            v((line, fold, half), BF16),
            v((line, fold, half), BF16),
            v((line, fold, half), F32),
            v((line, fold, half), BF16),
            v((line, fold, half), BF16),
            dma((RING + HELD,)),
            along, along, along, along, along,
            dma((sides, line, PIECES)), dma((sides, line, PIECES)),
            dma((chunks,)), dma((chunks,)), dma((BOTH,)), dma((BOTH,)), dma((chunks,)), dma((chunks,)),
            dma((members,)), dma((members,)), dma((2,)),
            dma((line,)), dma((line,)), dma((line,)), dma((line,)), dma((line,)), dma((line,)),
        ],
        compiler_params=pltpu.CompilerParams(
            collective_id=0, has_side_effects=True, vmem_limit_bytes=62 * 1024 * 1024
        ),
        name="step",
    )(hidden, head_weights, token_ids, kl_weight, advantage)


def fits(quarter, line, hidden, head_weights):
    rows, feats = hidden.shape
    depth, width = head_weights.shape
    return (
        quarter == 4
        and line >= 2
        and rows * quarter == 2 * LANES
        and width % WIDTH == 0
        and rows % (16 * PIECES) == 0
        and width // WIDTH >= 2 * HELD + 2 * BOTH
        and AHEAD < HELD
        and line + 4 <= HELD
        and depth % (8 * LANES) == 0
        and feats % 32 == 0
        and feats * line == depth
    )


def device_step(hidden, head_weights, token_ids, kl_weight, advantage):
    quarter, line = lax.axis_size("wide") // 2, lax.axis_size("narrow")
    run = fused if fits(quarter, line, hidden, head_weights) else body
    return run(hidden, head_weights, token_ids, kl_weight, advantage)


def solution(mesh):
    return jax.shard_map(
        device_step,
        mesh=mesh,
        in_specs=(P("wide", "narrow"), P(None, ("wide", "narrow")), P(), P(), P()),
        out_specs=(P("narrow", "wide"), P(), P()),
        check_vma=False,
    )
```
